128 devices in a mesh: shard: 32 (over z, y, x_lo), model: 4 (over x_hi, core).
Axes of the slice: x: 4 (x_hi: 2, x_lo: 2; x = x_hi * 2 + x_lo), y: 4, z: 4, core: 2. Of those that a mesh axis runs over, the one named last changes fastest.
Arguments:
- w_query: bfloat16 [12288, 12288], P('shard', 'model'), may hold values from -0.109375 to 0.109375
- low_query: bfloat16 [12288, 16], P('shard'), may hold values from -0.0546875 to 0.0546875
- high_query: bfloat16 [16, 12288], P(None, 'model'), may hold values from -1.5 to 1.5
- w_key: bfloat16 [12288, 12288], P('shard', 'model'), may hold values from -0.109375 to 0.109375
- low_key: bfloat16 [12288, 16], P('shard'), may hold values from -0.0546875 to 0.0546875
- high_key: bfloat16 [16, 12288], P(None, 'model'), may hold values from -1.5 to 1.5
- w_value: bfloat16 [12288, 12288], P('shard', 'model'), may hold values from -0.109375 to 0.109375
- low_value: bfloat16 [12288, 16], P('shard'), may hold values from -0.0546875 to 0.0546875
- high_value: bfloat16 [16, 12288], P(None, 'model'), may hold values from -1.5 to 1.5
- norm_gain: float32 [12288], P('shard'), may hold values from 0.25 to 1.75
Outputs:
- final_query: bfloat16 [12288, 12288], P(None, ('model', 'shard'))
- final_key: bfloat16 [12288, 12288], P(None, ('model', 'shard'))
- final_value: bfloat16 [12288, 12288], P(None, ('model', 'shard'))
- scale_query: float32 [12288], P(('model', 'shard'))
- scale_key: float32 [12288], P(('model', 'shard'))
- scale_value: float32 [12288], P(('model', 'shard'))
The draws below stay inside these ranges and needn't reach their ends.
All inputs are finite; a program needn't handle non-finite values. Where the reference program divides by a largest or mean magnitude, that divisor is 1e-20 or more.
Results may differ from the reference program's by a relative error of at most 0.001.
Values may be sent and summed in bfloat16 or wider, within the bound.
No kernel may reach another device: no remote copies, remote signals or barrier semaphores. Data moves between devices by JAX's collectives and lax.ppermute only.
A program may use at most 128 MiB of HBM per device.

```python
import jax
import jax.numpy as jnp

D_MODEL = 12288
Q_DIM = 12288
KV_DIM = 12288
RANK = 16


def with_spikes(values, key, source, target, blocks, factor):
    def block_of(dim):
        return (jnp.arange(values.shape[dim]) // (values.shape[dim] // blocks)).reshape((-1,) + (1,) * (values.ndim - 1 - dim))

    near = jax.random.permutation(key, blocks)[block_of(target)]
    second = (block_of(target) + blocks // 2) % blocks
    return jnp.where((block_of(source) == near) | (block_of(source) == second), factor * values, values)


def shard_levels(stream_key, extent, split, low, largest):
    gain, own = 1.0, jax.random.fold_in(stream_key, 6)
    for position, blocks in split:
        steps = jnp.exp(jax.random.uniform(jax.random.fold_in(own, position), (blocks,), jnp.float32, low / len(split), largest / len(split)))
        gain = gain * jnp.repeat(steps, extent[position] // blocks).reshape([-1 if axis == position else 1 for axis in range(len(extent))])
    return gain


def normal_values(stream_key, extent, width, reach, shards=(), dtype=jnp.bfloat16):
    entries = jax.random.normal(stream_key, extent, jnp.float32) * width
    if len(shards) > 0:
        entries = shard_levels(stream_key, extent, shards, -0.22, 0.18) * entries
    return jnp.clip(entries, min=-reach, max=reach).astype(dtype)


def heavy_noise(rng, extent, width, reach, cuts, heavy, kind=jnp.bfloat16):
    values = width * jax.random.normal(rng, extent, jnp.float32)
    if cuts:
        values = values * shard_levels(rng, extent, cuts, -0.22, 0.18)
    return jnp.clip(with_spikes(values, jax.random.fold_in(rng, 3), *heavy), -reach, reach).astype(kind)


def setup_inputs(seed: int = 0) -> dict:
    streams_of = jax.random.split(jax.random.key(seed), 11)
    w_query = heavy_noise(streams_of[0], (D_MODEL, Q_DIM), D_MODEL ** -0.5, 0.109375, ((0, 32), (1, 4)), (0, 1, 32, 2.75))
    low_query = normal_values(streams_of[1], (D_MODEL, RANK), D_MODEL ** -0.5, 0.0546875, ((0, 32),))
    high_query = normal_values(streams_of[2], (RANK, Q_DIM), RANK ** -0.5, 1.5, ((1, 4),))
    w_key = heavy_noise(streams_of[3], (D_MODEL, KV_DIM), D_MODEL ** -0.5, 0.109375, ((0, 32), (1, 4)), (0, 1, 32, 2.75))
    low_key = normal_values(streams_of[4], (D_MODEL, RANK), D_MODEL ** -0.5, 0.0546875, ((0, 32),))
    high_key = normal_values(streams_of[5], (RANK, KV_DIM), RANK ** -0.5, 1.5, ((1, 4),))
    w_value = heavy_noise(streams_of[6], (D_MODEL, KV_DIM), D_MODEL ** -0.5, 0.109375, ((0, 32), (1, 4)), (0, 1, 32, 2.75))
    low_value = normal_values(streams_of[7], (D_MODEL, RANK), D_MODEL ** -0.5, 0.0546875, ((0, 32),))
    high_value = normal_values(streams_of[8], (RANK, KV_DIM), RANK ** -0.5, 1.5, ((1, 4),))
    norm_gain = jnp.clip(1.0 + 0.15 * jax.random.normal(streams_of[9], (D_MODEL,), jnp.float32), 0.25, 1.75)
    return dict(w_query=w_query, low_query=low_query, high_query=high_query, w_key=w_key, low_key=low_key, high_key=high_key, w_value=w_value, low_value=low_value, high_value=high_value, norm_gain=norm_gain)


mix_rate = 1.0


def reference(w_query, low_query, high_query, w_key, low_key, high_key, w_value, low_value, high_value, norm_gain):
    result_query = w_query.astype(jnp.float32) + mix_rate * jnp.dot(low_query, high_query, preferred_element_type=jnp.float32)
    result_key = w_key.astype(jnp.float32) + mix_rate * jnp.dot(low_key, high_key, preferred_element_type=jnp.float32)
    result_value = w_value.astype(jnp.float32) + mix_rate * jnp.dot(low_value, high_value, preferred_element_type=jnp.float32)
    result_gained_query = result_query * norm_gain[:, None]
    result_gained_key = result_key * norm_gain[:, None]
    result_gained_value = result_value * norm_gain[:, None]
    scale_query = jnp.max(jnp.abs(result_gained_query), axis=0)
    final_query = (result_gained_query / scale_query).astype(jnp.bfloat16)
    scale_key = jnp.max(jnp.abs(result_gained_key), axis=0)
    final_key = (result_gained_key / scale_key).astype(jnp.bfloat16)
    scale_value = jnp.max(jnp.abs(result_gained_value), axis=0)
    final_value = (result_gained_value / scale_value).astype(jnp.bfloat16)
    return final_query, final_key, final_value, scale_query, scale_key, scale_value
```

```python
import functools

import jax
import jax.numpy as jnp
from jax import lax
from jax.experimental import pallas as pl
from jax.experimental.pallas import tpu as pltpu
from jax.sharding import PartitionSpec as P

GROUP = 4
TAIL = 8
LANES = 128


def pack_kernel(*refs, cols, rank):
    ws, lows, gain, out = refs[:3], refs[3:6], refs[6], refs[7]
    inbox, lowbox, gbox, insem, lowsem = refs[8:]
    each = cols + rank
    wide = GROUP * cols
    groups = out.shape[0] // GROUP
    fetch = [
        [
            pltpu.make_async_copy(
                w.at[:, i * wide : (i + 1) * wide], inbox.at[m, i], insem.at[i, m]
            )
            for m, w in enumerate(ws)
        ]
        for i in range(groups)
    ]
    small = [
        pltpu.make_async_copy(low, lowbox.at[m], lowsem.at[m]) for m, low in enumerate(lows)
    ]
    small.append(pltpu.make_async_copy(gain, gbox, lowsem.at[3]))
    for copy in small:
        copy.start()
    for i in range(groups):
        for copy in fetch[i]:
            copy.start()
    for copy in small:
        copy.wait()
    g = gbox[...].reshape(1, -1)
    first = g.astype(jnp.bfloat16)
    rest = g - first.astype(jnp.float32)
    second = rest.astype(jnp.bfloat16)
    third = (rest - second.astype(jnp.float32)).astype(jnp.bfloat16)
    none = jnp.zeros((TAIL - 3, g.shape[1]), jnp.bfloat16)
    parts = jnp.concatenate([first, second, third, none], 0)
    for i in range(groups):
        for m in range(3):
            fetch[i][m].wait()
            turned = inbox[m, i].T
            for p in range(GROUP):
                at = i * GROUP + p
                out[at, m * each : m * each + cols, :] = turned[p * cols : (p + 1) * cols, :]
                out[at, m * each + cols : (m + 1) * each, :] = lowbox[m]
        for p in range(GROUP):
            out[i * GROUP + p, 3 * each :, :] = parts


def far(x):
    return pltpu.with_memory_space_constraint(x, pltpu.HBM)


def pack(weights, lows, gain, peers):
    rows, width = weights[0].shape
    rank = lows[0].shape[0]
    cols = width // peers
    tall = 3 * (cols + rank) + TAIL
    groups = peers // GROUP
    hbm = pl.BlockSpec(memory_space=pltpu.HBM)
    vmem = pl.BlockSpec(memory_space=pltpu.VMEM)
    return pl.pallas_call(
        functools.partial(pack_kernel, cols=cols, rank=rank),
        in_specs=[hbm] * 7,
        out_specs=vmem,
        out_shape=jax.ShapeDtypeStruct((peers, tall, rows), jnp.bfloat16),
        scratch_shapes=[
            pltpu.VMEM((3, groups, rows, GROUP * cols), jnp.bfloat16),
            pltpu.VMEM((3, rank, rows), jnp.bfloat16),
            pltpu.VMEM((rows,), jnp.float32),
            pltpu.SemaphoreType.DMA((groups, 3)),
            pltpu.SemaphoreType.DMA((4,)),
        ],
        compiler_params=pltpu.CompilerParams(vmem_limit_bytes=24 * 2**20),
        name="pack",
    )(*map(far, weights), *map(far, lows), far(gain))


def merge_kernel(got, *refs, cols):
    highs, finals, scales = refs[:3], refs[3:6], refs[6:9]
    highbox, wide, outbox, insem, outsem = refs[9:]
    rank, width = highs[0].shape
    each = cols + rank
    peers, tall, rows = got.shape
    start = lax.axis_index("shard") * cols
    base = jnp.minimum(start // LANES, width // LANES - 2) * LANES
    base = pl.multiple_of(base, LANES)
    fetch = [
        pltpu.make_async_copy(high.at[:, pl.ds(base, 2 * LANES)], highbox.at[m], insem.at[m])
        for m, high in enumerate(highs)
    ]
    for copy in fetch:
        copy.start()
    send = [
        [
            pltpu.make_async_copy(
                outbox.at[m, c * 32 : (c + 1) * 32], finals[m].at[c * 32 : (c + 1) * 32], outsem.at[m, c]
            )
            for c in range(cols // 32)
        ]
        for m in range(3)
    ]
    at_col = lax.broadcasted_iota(jnp.int32, (cols, 2 * LANES), 0) + (start - base)
    pick = (at_col == lax.broadcasted_iota(jnp.int32, (cols, 2 * LANES), 1)).astype(jnp.bfloat16)
    same = (
        lax.broadcasted_iota(jnp.int32, (cols, cols), 0)
        == lax.broadcasted_iota(jnp.int32, (cols, cols), 1)
    ).astype(jnp.bfloat16)
    for copy in fetch:
        copy.wait()
    for m in range(3):
        mine = lax.dot_general(
            pick, highbox[m], (((1,), (1,)), ((), ())), preferred_element_type=jnp.float32
        ).astype(jnp.bfloat16)
        mix = jnp.concatenate([same, mine], 1)
        top = jnp.zeros((cols, rows), jnp.float32)
        for p in range(peers):
            g = got[p, 3 * each : tall, :].astype(jnp.float32)
            gain = g[0:1, :] + g[1:2, :] + g[2:3, :]
            value = (
                jnp.dot(mix, got[p, m * each : (m + 1) * each, :], preferred_element_type=jnp.float32)
                * gain
            )
            wide[:, p * rows : (p + 1) * rows] = value
            top = jnp.maximum(top, jnp.abs(value))
        scale = jnp.max(top, axis=1, keepdims=True)
        scales[m][...] = jnp.broadcast_to(scale, (cols, LANES)).T[0:1, :]
        down = 1.0 / scale
        for c in range(cols // 32):
            part = slice(c * 32, (c + 1) * 32)
            for p in range(peers):
                at = slice(p * rows, (p + 1) * rows)
                outbox[m, part, at] = (wide[part, at] * down[part]).astype(jnp.bfloat16)
            send[m][c].start()
    for copies in send:
        for copy in copies:
            copy.wait()


def merge(got, highs, cols):
    peers, _, rows = got.shape
    rank = highs[0].shape[0]
    whole = jax.ShapeDtypeStruct((cols, peers * rows), jnp.bfloat16)
    line = jax.ShapeDtypeStruct((1, cols), jnp.float32)
    hbm = pl.BlockSpec(memory_space=pltpu.HBM)
    vmem = pl.BlockSpec(memory_space=pltpu.VMEM)
    return pl.pallas_call(
        functools.partial(merge_kernel, cols=cols),
        in_specs=[vmem] + [hbm] * 3,
        out_specs=[hbm] * 3 + [vmem] * 3,
        out_shape=[whole] * 3 + [line] * 3,
        scratch_shapes=[
            pltpu.VMEM((3, rank, 2 * LANES), jnp.bfloat16),
            pltpu.VMEM((cols, peers * rows), jnp.float32),
            pltpu.VMEM((3, cols, peers * rows), jnp.bfloat16),
            pltpu.SemaphoreType.DMA((3,)),
            pltpu.SemaphoreType.DMA((3, cols // 32)),
        ],
        compiler_params=pltpu.CompilerParams(vmem_limit_bytes=24 * 2**20),
        name="merge",
    )(got, *map(far, highs))


def on_device(
    w_query,
    low_query,
    high_query,
    w_key,
    low_key,
    high_key,
    w_value,
    low_value,
    high_value,
    norm_gain,
):
    peers = lax.axis_size("shard")
    cols = w_query.shape[1] // peers
    sent = pack(
        (w_query, w_key, w_value), (low_query.T, low_key.T, low_value.T), norm_gain, peers
    )
    got = lax.all_to_all(sent, "shard", split_axis=0, concat_axis=0, tiled=True)
    *finals, scale_query, scale_key, scale_value = merge(
        got, (high_query, high_key, high_value), cols
    )
    return (
        *(f.T for f in finals),
        scale_query.reshape(-1),
        scale_key.reshape(-1),
        scale_value.reshape(-1),
    )


def solution(mesh):
    return jax.shard_map(
        on_device,
        mesh=mesh,
        in_specs=(
            P("shard", "model"),
            P("shard", None),
            P(None, "model"),
            P("shard", "model"),
            P("shard", None),
            P(None, "model"),
            P("shard", "model"),
            P("shard", None),
            P(None, "model"),
            P("shard"),
        ),
        out_specs=(
            P(None, ("model", "shard")),
            P(None, ("model", "shard")),
            P(None, ("model", "shard")),
            P(("model", "shard")),
            P(("model", "shard")),
            P(("model", "shard")),
        ),
        check_vma=False,
    )
```

```python
import functools

import jax
import jax.numpy as jnp
from jax import lax
from jax.experimental import pallas as pl
from jax.experimental.pallas import tpu as pltpu
from jax.sharding import PartitionSpec as P

GROUP = 4
TAIL = 8
LANES = 128


def split3(g):
    first = g.astype(jnp.bfloat16)
    rest = g - first.astype(jnp.float32)
    second = rest.astype(jnp.bfloat16)
    third = (rest - second.astype(jnp.float32)).astype(jnp.bfloat16)
    none = jnp.zeros((TAIL - 3, g.shape[1]), jnp.bfloat16)
    return jnp.concatenate([first, second, third, none], 0)


def pack_kernel(*refs, cols, rank):
    ws, lows, gain, highs, out, mix = refs[:3], refs[3:6], refs[6], refs[7:10], refs[10], refs[11]
    inbox, lowbox, gbox, highbox, insem, lowsem = refs[12:]
    each = cols + rank
    wide = GROUP * cols
    groups = out.shape[0] // GROUP
    width = ws[0].shape[1]
    start = lax.axis_index("shard") * cols
    base = jnp.minimum(start // LANES, width // LANES - 2) * LANES
    base = pl.multiple_of(base, LANES)
    fetch = [
        [
            pltpu.make_async_copy(
                w.at[:, i * wide : (i + 1) * wide], inbox.at[m, i], insem.at[i, m]
            )
            for m, w in enumerate(ws)
        ]
        for i in range(groups)
    ]
    small = [
        pltpu.make_async_copy(low, lowbox.at[m], lowsem.at[m]) for m, low in enumerate(lows)
    ]
    small += [
        pltpu.make_async_copy(high.at[:, pl.ds(base, 2 * LANES)], highbox.at[m], lowsem.at[3 + m])
        for m, high in enumerate(highs)
    ]
    small.append(pltpu.make_async_copy(gain, gbox, lowsem.at[6]))
    for i in range(groups):
        for copy in fetch[i]:
            copy.start()
        if i == 1:
            for copy in small:
                copy.start()
    for i in range(groups):
        for m in range(3):
            fetch[i][m].wait()
            turned = inbox[m, i].T
            for p in range(GROUP):
                at = i * GROUP + p
                out[at, m * each : m * each + cols, :] = turned[p * cols : (p + 1) * cols, :]
        if i == 2:
            for copy in small:
                copy.wait()
            parts = split3(gbox[...].reshape(1, -1))
            at_col = lax.broadcasted_iota(jnp.int32, (cols, 2 * LANES), 0) + (start - base)
            pick = at_col == lax.broadcasted_iota(jnp.int32, (cols, 2 * LANES), 1)
            pick = pick.astype(jnp.bfloat16)
            same = (
                lax.broadcasted_iota(jnp.int32, (cols, cols), 0)
                == lax.broadcasted_iota(jnp.int32, (cols, cols), 1)
            ).astype(jnp.bfloat16)
            for m in range(3):
                mine = lax.dot_general(
                    pick, highbox[m], (((1,), (1,)), ((), ())), preferred_element_type=jnp.float32
                )
                mix[m] = jnp.concatenate([same, mine.astype(jnp.bfloat16)], 1)
        if i == 3:
            for at in range(groups * GROUP):
                for m in range(3):
                    out[at, m * each + cols : (m + 1) * each, :] = lowbox[m]
                out[at, 3 * each :, :] = parts


def far(x):
    return pltpu.with_memory_space_constraint(x, pltpu.HBM)


def pack(weights, lows, gain, highs, peers):
    rows, width = weights[0].shape
    rank = lows[0].shape[0]
    cols = width // peers
    tall = 3 * (cols + rank) + TAIL
    groups = peers // GROUP
    hbm = pl.BlockSpec(memory_space=pltpu.HBM)
    vmem = pl.BlockSpec(memory_space=pltpu.VMEM)
    return pl.pallas_call(
        functools.partial(pack_kernel, cols=cols, rank=rank),
        in_specs=[hbm] * 10,
        out_specs=[vmem] * 2,
        out_shape=[
            jax.ShapeDtypeStruct((peers, tall, rows), jnp.bfloat16),
            jax.ShapeDtypeStruct((3, cols, cols + rank), jnp.bfloat16),
        ],
        scratch_shapes=[
            pltpu.VMEM((3, groups, rows, GROUP * cols), jnp.bfloat16),
            pltpu.VMEM((3, rank, rows), jnp.bfloat16),
            pltpu.VMEM((rows,), jnp.float32),
            pltpu.VMEM((3, rank, 2 * LANES), jnp.bfloat16),
            pltpu.SemaphoreType.DMA((groups, 3)),
            pltpu.SemaphoreType.DMA((7,)),
        ],
        compiler_params=pltpu.CompilerParams(vmem_limit_bytes=24 * 2**20),
        name="pack",
    )(*map(far, weights), *map(far, lows), far(gain), *map(far, highs))


def merge_kernel(got, mix, *refs):
    finals, scales = refs[:3], refs[3:6]
    wide, outbox, outsem = refs[6:]
    _, cols, each = mix.shape
    peers, tall, rows = got.shape
    send = [
        [
            pltpu.make_async_copy(
                outbox.at[m, c * 32 : (c + 1) * 32], finals[m].at[c * 32 : (c + 1) * 32], outsem.at[m, c]
            )
            for c in range(cols // 32)
        ]
        for m in range(3)
    ]
    for m in range(3):
        top = jnp.zeros((cols, rows), jnp.float32)
        for p in range(peers):
            g = got[p, 3 * each : tall, :].astype(jnp.float32)
            gain = g[0:1, :] + g[1:2, :] + g[2:3, :]
            value = (
                jnp.dot(mix[m], got[p, m * each : (m + 1) * each, :], preferred_element_type=jnp.float32)
                * gain
            )
            wide[:, p * rows : (p + 1) * rows] = value
            top = jnp.maximum(top, jnp.abs(value))
        scale = jnp.max(top, axis=1, keepdims=True)
        scales[m][...] = jnp.broadcast_to(scale, (cols, LANES)).T[0:1, :]
        down = 1.0 / scale
        for c in range(cols // 32):
            part = slice(c * 32, (c + 1) * 32)
            for p in range(peers):
                at = slice(p * rows, (p + 1) * rows)
                outbox[m, part, at] = (wide[part, at] * down[part]).astype(jnp.bfloat16)
            send[m][c].start()
    for copies in send:
        for copy in copies:
            copy.wait()


def merge(got, mix):
    peers, _, rows = got.shape
    _, cols, _ = mix.shape
    whole = jax.ShapeDtypeStruct((cols, peers * rows), jnp.bfloat16)
    line = jax.ShapeDtypeStruct((1, cols), jnp.float32)
    hbm = pl.BlockSpec(memory_space=pltpu.HBM)
    vmem = pl.BlockSpec(memory_space=pltpu.VMEM)
    return pl.pallas_call(
        merge_kernel,
        in_specs=[vmem] * 2,
        out_specs=[hbm] * 3 + [vmem] * 3,
        out_shape=[whole] * 3 + [line] * 3,
        scratch_shapes=[
            pltpu.VMEM((cols, peers * rows), jnp.float32),
            pltpu.VMEM((3, cols, peers * rows), jnp.bfloat16),
            pltpu.SemaphoreType.DMA((3, cols // 32)),
        ],
        compiler_params=pltpu.CompilerParams(vmem_limit_bytes=24 * 2**20),
        name="merge",
    )(got, mix)


def on_device(
    w_query,
    low_query,
    high_query,
    w_key,
    low_key,
    high_key,
    w_value,
    low_value,
    high_value,
    norm_gain,
):
    sent, mix = pack(
        (w_query, w_key, w_value),
        (low_query.T, low_key.T, low_value.T),
        norm_gain,
        (high_query, high_key, high_value),
        lax.axis_size("shard"),
    )
    got = lax.all_to_all(sent, "shard", split_axis=0, concat_axis=0, tiled=True)
    *finals, scale_query, scale_key, scale_value = merge(got, mix)
    return (
        *(f.T for f in finals),
        scale_query.reshape(-1),
        scale_key.reshape(-1),
        scale_value.reshape(-1),
    )


def solution(mesh):
    return jax.shard_map(
        on_device,
        mesh=mesh,
        in_specs=(
            P("shard", "model"),
            P("shard", None),
            P(None, "model"),
            P("shard", "model"),
            P("shard", None),
            P(None, "model"),
            P("shard", "model"),
            P("shard", None),
            P(None, "model"),
            P("shard"),
        ),
        out_specs=(
            P(None, ("model", "shard")),
            P(None, ("model", "shard")),
            P(None, ("model", "shard")),
            P(("model", "shard")),
            P(("model", "shard")),
            P(("model", "shard")),
        ),
        check_vma=False,
    )
```

```python
import functools

import jax
import jax.numpy as jnp
from jax import lax
from jax.experimental import pallas as pl
from jax.experimental.pallas import tpu as pltpu
from jax.sharding import PartitionSpec as P


SIDE = 4
PLANE = 8
PEERS = SIDE * PLANE
GROUP = 4
LANES = 128
EARLY = 32
TAIL = 8
HBM = pl.BlockSpec(memory_space=pltpu.HBM)
VMEM = pl.BlockSpec(memory_space=pltpu.VMEM)
PARAMS = pltpu.CompilerParams(vmem_limit_bytes=30 * 2**20)


def moved(place, dz, i):
    dy, dx = i // 2, i % 2
    z, y, x = place // PLANE, (place // 2) % SIDE, place % 2
    return ((z + dz) % SIDE) * PLANE + ((y + dy) % SIDE) * 2 + (x + dx) % 2


def came_from(place, dz, i):
    return moved(place, -dz % SIDE, (-(i // 2) % SIDE) * 2 + i % 2)


def far(x):
    return pltpu.with_memory_space_constraint(x, pltpu.HBM)


def shape(*dims):
    return jax.ShapeDtypeStruct(dims, jnp.bfloat16)


def split3(g):
    first = g.astype(jnp.bfloat16)
    rest = g - first.astype(jnp.float32)
    second = rest.astype(jnp.bfloat16)
    third = (rest - second.astype(jnp.float32)).astype(jnp.bfloat16)
    none = jnp.zeros((TAIL - 3, g.shape[1]), jnp.bfloat16)
    return jnp.concatenate([first, second, third, none], 0)


def fetches(ws, inbox, insem):
    groups = PEERS // GROUP
    wide = ws[0].shape[1] // groups
    return [
        [
            pltpu.make_async_copy(
                w.at[:, i * wide : (i + 1) * wide], inbox.at[m, i], insem.at[i, m]
            )
            for m, w in enumerate(ws)
        ]
        for i in range(groups)
    ]


def turn_group(i, fetch, inbox, turn, cols):
    for m, copy in enumerate(fetch[i]):
        copy.wait()
        turned = inbox[m, i].T
        for p in range(GROUP):
            turn[i * GROUP + p, m * cols : (m + 1) * cols, :] = turned[p * cols : (p + 1) * cols, :]


def pack_ac_kernel(wq, wk, low, *refs, cols):
    lot_a, lot_c = refs[:SIDE], refs[SIDE : SIDE + PLANE]
    inbox, turn, lowbox, insem, lowsem = refs[SIDE + PLANE :]
    first = cols + EARLY
    rest = cols - EARLY
    place = lax.axis_index("shard")
    small = pltpu.make_async_copy(low, lowbox, lowsem)
    fetch = fetches((wq, wk), inbox, insem)
    for copies in fetch:
        for copy in copies:
            copy.start()
    small.start()
    for i in range(PEERS // GROUP):
        turn_group(i, fetch, inbox, turn, cols)
    small.wait()
    for dz in range(SIDE):
        lot_a[dz][PLANE * first :, :] = lowbox[...]
        for i in range(PLANE):
            to = moved(place, dz, i)
            lot_a[dz][i * first : (i + 1) * first, :] = turn[to, 0:first, :]
            lot_c[i][dz * rest : (dz + 1) * rest, :] = turn[to, first:, :]


def pack_ac(w_query, w_key, low):
    rows, width = w_query.shape
    rank = low.shape[0]
    cols = width // PEERS
    groups = PEERS // GROUP
    out = [shape(PLANE * (cols + EARLY) + rank, rows)] * SIDE
    out += [shape(SIDE * (cols - EARLY), rows)] * PLANE
    got = pl.pallas_call(
        functools.partial(pack_ac_kernel, cols=cols),
        in_specs=[HBM] * 3,
        out_specs=[VMEM] * len(out),
        out_shape=out,
        scratch_shapes=[
            pltpu.VMEM((2, groups, rows, GROUP * cols), jnp.bfloat16),
            pltpu.VMEM((PEERS, 2 * cols, rows), jnp.bfloat16),
            pltpu.VMEM((rank, rows), jnp.bfloat16),
            pltpu.SemaphoreType.DMA((groups, 2)),
            pltpu.SemaphoreType.DMA,
        ],
        compiler_params=PARAMS,
        name="pack_ac",
    )(far(w_query), far(w_key), far(low))
    return got[:SIDE], got[SIDE:]


def pack_b_kernel(wv, low_k, low_v, gain, *refs, cols):
    highs, lot, mix = refs[:3], refs[3 : 3 + PLANE], refs[3 + PLANE]
    inbox, turn, lowbox, gbox, highbox, insem, lowsem = refs[4 + PLANE :]
    width = wv.shape[1]
    place = lax.axis_index("shard")
    core = lax.axis_index("model") % 2
    start = place * cols
    base = jnp.minimum(start // LANES, width // LANES - 2) * LANES
    base = pl.multiple_of(base, LANES)
    fetch = fetches((wv,), inbox, insem)
    for copies in fetch:
        copies[0].start()
    small = [
        pltpu.make_async_copy(high.at[:, pl.ds(base, 2 * LANES)], highbox.at[m], lowsem.at[m])
        for m, high in enumerate(highs)
    ]
    small.append(pltpu.make_async_copy(gain, gbox, lowsem.at[3]))
    for copy in small:
        copy.start()
    even = pltpu.make_async_copy(low_k, lowbox, lowsem.at[4])
    odd = pltpu.make_async_copy(low_v, lowbox, lowsem.at[4])

    @pl.when(core == 0)
    def _():
        even.start()

    @pl.when(core == 1)
    def _():
        odd.start()

    for i in range(PEERS // GROUP):
        turn_group(i, fetch, inbox, turn, cols)
    for copy in (*small, even):
        copy.wait()
    at_col = lax.broadcasted_iota(jnp.int32, (cols, 2 * LANES), 0) + (start - base)
    pick = at_col == lax.broadcasted_iota(jnp.int32, (cols, 2 * LANES), 1)
    pick = pick.astype(jnp.bfloat16)
    same = (
        lax.broadcasted_iota(jnp.int32, (cols, cols), 0)
        == lax.broadcasted_iota(jnp.int32, (cols, cols), 1)
    ).astype(jnp.bfloat16)
    for m in range(3):
        own = lax.dot_general(
            pick, highbox[m], (((1,), (1,)), ((), ())), preferred_element_type=jnp.float32
        )
        mix[m] = jnp.concatenate([same, own.astype(jnp.bfloat16)], 1)
    parts = split3(gbox[...].reshape(1, -1))
    rank = lowbox.shape[0]
    for i in range(PLANE):
        for dz in range(SIDE):
            lot[i][dz * cols : (dz + 1) * cols, :] = turn[moved(place, dz, i)]
        lot[i][SIDE * cols : SIDE * cols + rank, :] = lowbox[...]
        lot[i][SIDE * cols + rank :, :] = parts


def pack_b(w_value, low_key, low_value, gain, highs):
    rows, width = w_value.shape
    rank = low_key.shape[0]
    cols = width // PEERS
    groups = PEERS // GROUP
    out = [shape(SIDE * cols + rank + TAIL, rows)] * PLANE + [shape(3, cols, cols + rank)]
    *lot, mix = pl.pallas_call(
        functools.partial(pack_b_kernel, cols=cols),
        in_specs=[HBM] * 7,
        out_specs=[VMEM] * len(out),
        out_shape=out,
        scratch_shapes=[
            pltpu.VMEM((1, groups, rows, GROUP * cols), jnp.bfloat16),
            pltpu.VMEM((PEERS, cols, rows), jnp.bfloat16),
            pltpu.VMEM((rank, rows), jnp.bfloat16),
            pltpu.VMEM((rows,), jnp.float32),
            pltpu.VMEM((3, rank, 2 * LANES), jnp.bfloat16),
            pltpu.SemaphoreType.DMA((groups, 1)),
            pltpu.SemaphoreType.DMA((5,)),
        ],
        compiler_params=PARAMS,
        name="pack_b",
    )(far(w_value), far(low_key), far(low_value), far(gain), *map(far, highs))
    return lot, mix


def repack(parts, moves, tall, count):
    def kernel(*refs):
        ins, outs = refs[: len(parts)], refs[len(parts) :]
        for k, to, j, at, n in moves:
            outs[k][to : to + n, :] = ins[j][at : at + n, :]

    out = [shape(tall, parts[0].shape[1])] * count
    return pl.pallas_call(
        kernel,
        in_specs=[VMEM] * len(parts),
        out_specs=[VMEM] * count,
        out_shape=out,
        compiler_params=PARAMS,
    )(*parts)


def place_all():
    return [(dz, i) for dz in range(SIDE) for i in range(PLANE)]


def finish(m, value_of, mix, scale_ref, wide, outbox, final, outsem):
    _, cols, _ = mix.shape
    rows = wide.shape[2]
    place = lax.axis_index("shard")
    top = jnp.zeros((cols, rows), jnp.float32)
    for dz, i in place_all():
        packed, g = value_of(dz, i)
        g = g.astype(jnp.float32)
        gain = g[0:1, :] + g[1:2, :] + g[2:3, :]
        value = jnp.dot(mix[m], packed, preferred_element_type=jnp.float32) * gain
        wide[came_from(place, dz, i)] = value
        top = jnp.maximum(top, jnp.abs(value))
    scale = jnp.max(top, axis=1, keepdims=True)
    scale_ref[...] = jnp.broadcast_to(scale, (cols, LANES)).T[0:1, :]
    down = 1.0 / scale
    copies = []
    for c in range(cols // 32):
        part = slice(c * 32, (c + 1) * 32)
        for p in range(PEERS):
            outbox[part, p * rows : (p + 1) * rows] = (wide[p, part] * down[part]).astype(
                jnp.bfloat16
            )
        copies.append(pltpu.make_async_copy(outbox.at[part], final.at[part], outsem.at[c]))
        copies[-1].start()
    return copies


def merge_v_kernel(*refs):
    lot, theirs, mix, final, scale = refs[:SIDE], *refs[SIDE : SIDE + 4]
    wide, outbox, outsem = refs[SIDE + 4 :]
    _, cols, each = mix.shape
    rank = each - cols
    block = each + TAIL
    mine_is_value = lax.axis_index("model") % 2 == 1

    def value_of(dz, i):
        at = i * block
        other = (dz * PLANE + i) * (rank + TAIL)
        own = lot[dz][at + cols : at + each, :]
        low = jnp.where(mine_is_value, own, theirs[other : other + rank, :])
        packed = jnp.concatenate([lot[dz][at : at + cols, :], low], 0)
        return packed, lot[dz][at + each : at + block, :]

    for copy in finish(2, value_of, mix, scale, wide, outbox, final, outsem):
        copy.wait()


def merge_qk_kernel(*refs):
    lot_a, lot_c = refs[:PLANE], refs[PLANE : PLANE + SIDE]
    mine, theirs, mix, final_q, final_k, scale_q, scale_k = refs[PLANE + SIDE : PLANE + SIDE + 7]
    wide, outbox, outsem = refs[PLANE + SIDE + 7 :]
    _, cols, each = mix.shape
    rank = each - cols
    block = each + EARLY
    rest = cols - EARLY
    mine_is_key = lax.axis_index("model") % 2 == 0

    def gain_of(dz, i):
        at = (dz * PLANE + i) * (rank + TAIL)
        return mine[at + rank : at + rank + TAIL, :]

    def query_of(dz, i):
        return lot_a[i][dz * block : dz * block + each, :], gain_of(dz, i)

    def key_of(dz, i):
        at = (dz * PLANE + i) * (rank + TAIL)
        low = jnp.where(mine_is_key, mine[at : at + rank, :], theirs[at : at + rank, :])
        early = lot_a[i][dz * block + each : (dz + 1) * block, :]
        late = lot_c[dz][i * rest : (i + 1) * rest, :]
        return jnp.concatenate([early, late, low], 0), gain_of(dz, i)

    copies = finish(0, query_of, mix, scale_q, wide, outbox.at[0], final_q, outsem.at[0])
    copies += finish(1, key_of, mix, scale_k, wide, outbox.at[1], final_k, outsem.at[1])
    for copy in copies:
        copy.wait()


def merge(kernel, operands, mix, rows, count):
    _, cols, _ = mix.shape
    lead = () if count == 1 else (count,)
    return pl.pallas_call(
        kernel,
        in_specs=[VMEM] * (len(operands) + 1),
        out_specs=[HBM] * count + [VMEM] * count,
        out_shape=[shape(cols, PEERS * rows)] * count
        + [jax.ShapeDtypeStruct((1, cols), jnp.float32)] * count,
        scratch_shapes=[
            pltpu.VMEM((PEERS, cols, rows), jnp.float32),
            pltpu.VMEM((*lead, cols, PEERS * rows), jnp.bfloat16),
            pltpu.SemaphoreType.DMA((*lead, cols // 32)),
        ],
        compiler_params=PARAMS,
    )(*operands, mix)


def on_device(
    w_query,
    low_query,
    high_query,
    w_key,
    low_key,
    high_key,
    w_value,
    low_value,
    high_value,
    norm_gain,
):
    rows = w_query.shape[0]
    cols = w_query.shape[1] // PEERS
    rank = low_query.shape[1]
    each = cols + rank
    first, rest = cols + EARLY, cols - EARLY
    extra = rank + TAIL
    models = lax.axis_size("model")

    def leg(part, dz, i):
        pairs = [(s, moved(s, dz, i)) for s in range(PEERS)]
        return lax.ppermute(part, "shard", pairs)

    def along_z(lot):
        return [lot[0], *(leg(lot[dz], dz, 0) for dz in range(1, SIDE))]

    def in_plane(lot):
        return [lot[0], *(leg(lot[i], 0, i) for i in range(1, PLANE))]

    lot_a, lot_c = pack_ac(w_query, w_key, low_query.T)
    lot_b, mix = pack_b(
        w_value, low_key.T, low_value.T, norm_gain, (high_query, high_key, high_value)
    )
    lot_a = along_z(lot_a)
    lot_b = in_plane(lot_b)
    lot_c = in_plane(lot_c)
    moves = []
    for dz, i in place_all():
        moves.append((dz, i * (cols + extra), i, dz * cols, cols))
        moves.append((dz, i * (cols + extra) + cols, i, SIDE * cols, extra))
    lot_b = repack(lot_b, moves, PLANE * (cols + extra), SIDE)
    lot_b = along_z(lot_b)
    moves = []
    for dz, i in place_all():
        to = dz * (each + EARLY)
        moves.append((i, to, dz, i * first, cols))
        moves.append((i, to + cols, dz, PLANE * first, rank))
        moves.append((i, to + each, dz, i * first + cols, EARLY))
    lot_a = repack(lot_a, moves, SIDE * (each + EARLY), PLANE)
    lot_a = in_plane(lot_a)
    moves = [(dz, i * rest, i, dz * rest, rest) for dz, i in place_all()]
    lot_c = repack(lot_c, moves, PLANE * rest, SIDE)
    lot_c = along_z(lot_c)
    moves = [
        (0, (dz * PLANE + i) * extra, dz, i * (cols + extra) + cols, extra)
        for dz, i in place_all()
    ]
    (mine,) = repack(lot_b, moves, PEERS * extra, 1)
    theirs = lax.ppermute(mine, "model", [(m, m ^ 1) for m in range(models)])
    final_v, scale_v = merge(merge_v_kernel, (*lot_b, theirs), mix, rows, 1)
    final_q, final_k, scale_q, scale_k = merge(
        merge_qk_kernel, (*lot_a, *lot_c, mine, theirs), mix, rows, 2
    )
    return (
        final_q.T,
        final_k.T,
        final_v.T,
        scale_q.reshape(-1),
        scale_k.reshape(-1),
        scale_v.reshape(-1),
    )


def solution(mesh):
    return jax.shard_map(
        on_device,
        mesh=mesh,
        in_specs=(
            P("shard", "model"),
            P("shard", None),
            P(None, "model"),
            P("shard", "model"),
            P("shard", None),
            P(None, "model"),
            P("shard", "model"),
            P("shard", None),
            P(None, "model"),
            P("shard"),
        ),
        out_specs=(
            P(None, ("model", "shard")),
            P(None, ("model", "shard")),
            P(None, ("model", "shard")),
            P(("model", "shard")),
            P(("model", "shard")),
            P(("model", "shard")),
        ),
        check_vma=False,
    )
```

```python
import functools

import jax
import jax.numpy as jnp
from jax import lax
from jax.experimental import pallas as pl
from jax.experimental.pallas import tpu as pltpu
from jax.sharding import PartitionSpec as P


SIDE = 4
PLANE = 8
PEERS = SIDE * PLANE
GROUP = 4
LANES = 128
EARLY = 64
TAIL = 8
LATER_A = (0, 1, 3)
LATER_B = (0, 1, 2, 3, 6, 7)
HBM = pl.BlockSpec(memory_space=pltpu.HBM)
VMEM = pl.BlockSpec(memory_space=pltpu.VMEM)
PARAMS = pltpu.CompilerParams(vmem_limit_bytes=30 * 2**20)


def moved(place, dz, i):
    dy, dx = i // 2, i % 2
    z, y, x = place // PLANE, (place // 2) % SIDE, place % 2
    return ((z + dz) % SIDE) * PLANE + ((y + dy) % SIDE) * 2 + (x + dx) % 2


def came_from(place, dz, i):
    return moved(place, -dz % SIDE, (-(i // 2) % SIDE) * 2 + i % 2)


def far(x):
    return pltpu.with_memory_space_constraint(x, pltpu.HBM)


def shape(*dims):
    return jax.ShapeDtypeStruct(dims, jnp.bfloat16)


def split3(g):
    first = g.astype(jnp.bfloat16)
    rest = g - first.astype(jnp.float32)
    second = rest.astype(jnp.bfloat16)
    third = (rest - second.astype(jnp.float32)).astype(jnp.bfloat16)
    none = jnp.zeros((TAIL - 3, g.shape[1]), jnp.bfloat16)
    return jnp.concatenate([first, second, third, none], 0)


def low_of(core, low_k, low_v, lowbox, sem):
    even = pltpu.make_async_copy(low_k, lowbox, sem)
    odd = pltpu.make_async_copy(low_v, lowbox, sem)

    @pl.when(core == 0)
    def _():
        even.start()

    @pl.when(core == 1)
    def _():
        odd.start()

    return even


def turned(block, cols):
    t = block.T
    return [t[p * cols : (p + 1) * cols, :] for p in range(GROUP)]


def fill_b(lot, dz, weights, cols):
    lot[dz * cols : (dz + 1) * cols, :] = weights


def fill_b_tail(lot, low, parts, cols):
    rank = low.shape[0]
    lot[SIDE * cols : SIDE * cols + rank, :] = low
    lot[SIDE * cols + rank :, :] = parts


def pack_first_kernel(wq, wk, wv, low_q, low_k, low_v, gain, lot_a, b4, b5, *refs, cols):
    inbox, vbox, turn, vturn, qbox, lowbox, gbox, insem, vsem, lowsem = refs
    wide = GROUP * cols
    first = cols + EARLY
    place = lax.axis_index("shard")
    core = lax.axis_index("model") % 2
    z, y, x = place // PLANE, (place // 2) % SIDE, place % 2
    copies = []
    for h in range(2):
        at = pl.multiple_of((((z + 2) % SIDE) * 2 + h) * wide, LANES)
        for m, w in enumerate((wq, wk)):
            copies.append(
                pltpu.make_async_copy(w.at[:, pl.ds(at, wide)], inbox.at[m, h], insem.at[m, h])
            )
            copies[-1].start()
    vcopies = []
    for dz in range(SIDE):
        at = pl.multiple_of((((z + dz) % SIDE) * 2 + ((y + 2) % SIDE) // 2) * wide, LANES)
        vcopies.append(pltpu.make_async_copy(wv.at[:, pl.ds(at, wide)], vbox.at[dz], vsem.at[dz]))
        vcopies[-1].start()
    small = [
        pltpu.make_async_copy(low_q, qbox, lowsem.at[0]),
        pltpu.make_async_copy(gain, gbox, lowsem.at[1]),
    ]
    for copy in small:
        copy.start()
    small.append(low_of(core, low_k, low_v, lowbox, lowsem.at[2]))
    for copy in copies:
        copy.wait()
    for m in range(2):
        for h in range(2):
            for p, part in enumerate(turned(inbox[m, h], cols)):
                turn[h * GROUP + p, m * cols : (m + 1) * cols, :] = part
    for i in range(PLANE):
        to = moved(place, 0, i) % PLANE
        lot_a[i * first : (i + 1) * first, :] = turn[to, 0:first, :]
    for dz in range(SIDE):
        vcopies[dz].wait()
        for p, part in enumerate(turned(vbox[dz], cols)):
            vturn[dz * GROUP + p] = part
    for copy in small:
        copy.wait()
    lot_a[PLANE * first :, :] = qbox[...]
    parts = split3(gbox[...].reshape(1, -1))
    for dx, lot in enumerate((b4, b5)):
        for dz in range(SIDE):
            at = dz * GROUP + ((y + 2) % 2) * 2 + (x + dx) % 2
            fill_b(lot, dz, vturn[at], cols)
        fill_b_tail(lot, lowbox[...], parts, cols)


def pack_rest_kernel(wq, wk, wv, low_q, low_k, low_v, gain, *refs, cols):
    highs, refs = refs[:3], refs[3:]
    lot_a, refs = refs[: len(LATER_A)], refs[len(LATER_A) :]
    lot_b, refs = refs[: len(LATER_B)], refs[len(LATER_B) :]
    lot_c, mix, refs = refs[:PLANE], refs[PLANE], refs[PLANE + 1 :]
    inbox, turn, qbox, lowbox, gbox, highbox, insem, lowsem = refs
    wide = GROUP * cols
    first, rest = cols + EARLY, cols - EARLY
    width = wv.shape[1]
    place = lax.axis_index("shard")
    core = lax.axis_index("model") % 2
    start = place * cols
    base = jnp.minimum(start // LANES, width // LANES - 2) * LANES
    base = pl.multiple_of(base, LANES)
    copies = [
        [
            pltpu.make_async_copy(
                w.at[:, i * wide : (i + 1) * wide], inbox.at[m, i], insem.at[m, i]
            )
            for m, w in enumerate((wq, wk, wv))
        ]
        for i in range(PEERS // GROUP)
    ]
    for group in copies:
        for copy in group:
            copy.start()
    small = [
        pltpu.make_async_copy(high.at[:, pl.ds(base, 2 * LANES)], highbox.at[m], lowsem.at[m])
        for m, high in enumerate(highs)
    ]
    small.append(pltpu.make_async_copy(gain, gbox, lowsem.at[3]))
    small.append(pltpu.make_async_copy(low_q, qbox, lowsem.at[4]))
    for copy in small:
        copy.start()
    small.append(low_of(core, low_k, low_v, lowbox, lowsem.at[5]))
    for i in range(PEERS // GROUP):
        for m in range(3):
            copies[i][m].wait()
            for p, part in enumerate(turned(inbox[m, i], cols)):
                turn[i * GROUP + p, m * cols : (m + 1) * cols, :] = part
    for copy in small:
        copy.wait()
    at_col = lax.broadcasted_iota(jnp.int32, (cols, 2 * LANES), 0) + (start - base)
    pick = at_col == lax.broadcasted_iota(jnp.int32, (cols, 2 * LANES), 1)
    pick = pick.astype(jnp.bfloat16)
    same = (
        lax.broadcasted_iota(jnp.int32, (cols, cols), 0)
        == lax.broadcasted_iota(jnp.int32, (cols, cols), 1)
    ).astype(jnp.bfloat16)
    for m in range(3):
        own = lax.dot_general(
            pick, highbox[m], (((1,), (1,)), ((), ())), preferred_element_type=jnp.float32
        )
        mix[m] = jnp.concatenate([same, own.astype(jnp.bfloat16)], 1)
    parts = split3(gbox[...].reshape(1, -1))
    for lot, i in zip(lot_b, LATER_B):
        for dz in range(SIDE):
            fill_b(lot, dz, turn[moved(place, dz, i), 2 * cols : 3 * cols, :], cols)
        fill_b_tail(lot, lowbox[...], parts, cols)
    for lot, dz in zip(lot_a, LATER_A):
        lot[PLANE * first :, :] = qbox[...]
        for i in range(PLANE):
            lot[i * first : (i + 1) * first, :] = turn[moved(place, dz, i), 0:first, :]
    for i in range(PLANE):
        for dz in range(SIDE):
            lot_c[i][dz * rest : (dz + 1) * rest, :] = turn[
                moved(place, dz, i), first : 2 * cols, :
            ]


def pack(weights, lows, gain, highs):
    rows, width = weights[0].shape
    rank = lows[0].shape[0]
    cols = width // PEERS
    groups = PEERS // GROUP
    wide = GROUP * cols
    one_a = shape(PLANE * (cols + EARLY) + rank, rows)
    one_b = shape(SIDE * cols + rank + TAIL, rows)
    one_c = shape(SIDE * (cols - EARLY), rows)
    operands = [*map(far, weights), *map(far, lows), far(gain)]
    small = [
        pltpu.VMEM((rank, rows), jnp.bfloat16),
        pltpu.VMEM((rank, rows), jnp.bfloat16),
        pltpu.VMEM((rows,), jnp.float32),
    ]
    out = [one_a, one_b, one_b]
    lot_a, b4, b5 = pl.pallas_call(
        functools.partial(pack_first_kernel, cols=cols),
        in_specs=[HBM] * len(operands),
        out_specs=[VMEM] * len(out),
        out_shape=out,
        scratch_shapes=[
            pltpu.VMEM((2, 2, rows, wide), jnp.bfloat16),
            pltpu.VMEM((SIDE, rows, wide), jnp.bfloat16),
            pltpu.VMEM((PLANE, 2 * cols, rows), jnp.bfloat16),
            pltpu.VMEM((SIDE * GROUP, cols, rows), jnp.bfloat16),
            *small,
            pltpu.SemaphoreType.DMA((2, 2)),
            pltpu.SemaphoreType.DMA((SIDE,)),
            pltpu.SemaphoreType.DMA((3,)),
        ],
        compiler_params=PARAMS,
        name="pack_first",
    )(*operands)
    lots = {("a", 2): lot_a, ("b", 4): b4, ("b", 5): b5}
    operands += map(far, highs)
    names = [("a", k) for k in LATER_A] + [("b", k) for k in LATER_B]
    names += [("c", k) for k in range(PLANE)]
    out = [{"a": one_a, "b": one_b, "c": one_c}[name] for name, _ in names]
    out.append(shape(3, cols, cols + rank))
    *later, mix = pl.pallas_call(
        functools.partial(pack_rest_kernel, cols=cols),
        in_specs=[HBM] * len(operands),
        out_specs=[VMEM] * len(out),
        out_shape=out,
        scratch_shapes=[
            pltpu.VMEM((3, groups, rows, wide), jnp.bfloat16),
            pltpu.VMEM((PEERS, 3 * cols, rows), jnp.bfloat16),
            *small,
            pltpu.VMEM((3, rank, 2 * LANES), jnp.bfloat16),
            pltpu.SemaphoreType.DMA((3, groups)),
            pltpu.SemaphoreType.DMA((6,)),
        ],
        compiler_params=PARAMS,
        name="pack_rest",
    )(*operands)
    lots.update(zip(names, later))
    return (
        [lots["a", k] for k in range(SIDE)],
        [lots["b", k] for k in range(PLANE)],
        [lots["c", k] for k in range(PLANE)],
        mix,
    )


def repack_b(lot, cols, rank):
    rows = lot[0].shape[1]
    block = cols + rank
    tall = PLANE * block + 3 * PLANE

    def kernel(*refs):
        ins, outs = refs[:PLANE], refs[PLANE:]
        gains = [ref[SIDE * cols + rank :, :].astype(jnp.float32) for ref in ins]
        parts = [g[k : k + 1, :] for k in range(3) for g in gains]
        parts = jnp.concatenate(parts, 0).astype(jnp.bfloat16)
        for dz, out in enumerate(outs):
            for i, ref in enumerate(ins):
                at = i * block
                out[at : at + cols, :] = ref[dz * cols : (dz + 1) * cols, :]
                out[at + cols : at + block, :] = ref[SIDE * cols : SIDE * cols + rank, :]
            out[PLANE * block :, :] = parts

    return pl.pallas_call(
        kernel,
        in_specs=[VMEM] * PLANE,
        out_specs=[VMEM] * SIDE,
        out_shape=[shape(tall, rows)] * SIDE,
        compiler_params=PARAMS,
        name="repack_b",
    )(*lot)


def collect(lot, cols, rank):
    rows = lot[0].shape[1]
    block = cols + rank

    def kernel(*refs):
        ins, low, gain = refs[:SIDE], refs[SIDE], refs[SIDE + 1]
        for dz, ref in enumerate(ins):
            for i in range(PLANE):
                at = (dz * PLANE + i) * rank
                low[at : at + rank, :] = ref[i * block + cols : (i + 1) * block, :]
            g = ref[PLANE * block :, :].astype(jnp.float32)
            gain[dz * PLANE : (dz + 1) * PLANE, :] = (
                g[0:PLANE, :] + g[PLANE : 2 * PLANE, :] + g[2 * PLANE :, :]
            )

    return pl.pallas_call(
        kernel,
        in_specs=[VMEM] * SIDE,
        out_specs=[VMEM] * 2,
        out_shape=[shape(PEERS * rank, rows), jax.ShapeDtypeStruct((PEERS, rows), jnp.float32)],
        compiler_params=PARAMS,
        name="collect",
    )(*lot)


def repack(parts, moves, tall, count):
    def kernel(*refs):
        ins, outs = refs[: len(parts)], refs[len(parts) :]
        for k, to, j, at, n in moves:
            outs[k][to : to + n, :] = ins[j][at : at + n, :]

    out = [shape(tall, parts[0].shape[1])] * count
    return pl.pallas_call(
        kernel,
        in_specs=[VMEM] * len(parts),
        out_specs=[VMEM] * count,
        out_shape=out,
        compiler_params=PARAMS,
    )(*parts)


def place_all():
    return [(dz, i) for dz in range(SIDE) for i in range(PLANE)]


def merge(value_of, m, operands, gains, mix):
    _, cols, _ = mix.shape
    rows = gains.shape[1]
    count = len(operands)

    def kernel(*refs):
        ins, gain, both = refs[:count], refs[count], refs[count + 1]
        final, scale_ref, wide, outbox, outsem = refs[count + 2 :]
        place = lax.axis_index("shard")
        top = jnp.zeros((cols, rows), jnp.float32)
        for dz, i in place_all():
            at = dz * PLANE + i
            value = jnp.dot(both[m], value_of(ins, dz, i), preferred_element_type=jnp.float32)
            value = value * gain[at : at + 1, :]
            wide[came_from(place, dz, i)] = value
            top = jnp.maximum(top, jnp.abs(value))
        scale = jnp.max(top, axis=1, keepdims=True)
        scale_ref[...] = jnp.broadcast_to(scale, (cols, LANES)).T[0:1, :]
        down = 1.0 / scale
        copies = []
        for c in range(cols // 32):
            part = slice(c * 32, (c + 1) * 32)
            for p in range(PEERS):
                outbox[part, p * rows : (p + 1) * rows] = (wide[p, part] * down[part]).astype(
                    jnp.bfloat16
                )
            copies.append(pltpu.make_async_copy(outbox.at[part], final.at[part], outsem.at[c]))
            copies[-1].start()
        for copy in copies:
            copy.wait()

    return pl.pallas_call(
        kernel,
        in_specs=[VMEM] * (count + 2),
        out_specs=[HBM, VMEM],
        out_shape=[shape(cols, PEERS * rows), jax.ShapeDtypeStruct((1, cols), jnp.float32)],
        scratch_shapes=[
            pltpu.VMEM((PEERS, cols, rows), jnp.float32),
            pltpu.VMEM((cols, PEERS * rows), jnp.bfloat16),
            pltpu.SemaphoreType.DMA((cols // 32,)),
        ],
        compiler_params=PARAMS,
    )(*operands, gains, mix)


def on_device(
    w_query,
    low_query,
    high_query,
    w_key,
    low_key,
    high_key,
    w_value,
    low_value,
    high_value,
    norm_gain,
):
    cols = w_query.shape[1] // PEERS
    rank = low_query.shape[1]
    each = cols + rank
    first, rest = cols + EARLY, cols - EARLY
    models = lax.axis_size("model")

    def leg(part, dz, i):
        pairs = [(s, moved(s, dz, i)) for s in range(PEERS)]
        return lax.ppermute(part, "shard", pairs)

    def along_z(lot):
        return [lot[0], *(leg(lot[dz], dz, 0) for dz in range(1, SIDE))]

    def in_plane(lot):
        return [lot[0], *(leg(lot[i], 0, i) for i in range(1, PLANE))]

    lot_a, lot_b, lot_c, mix = pack(
        (w_query, w_key, w_value),
        (low_query.T, low_key.T, low_value.T),
        norm_gain,
        (high_query, high_key, high_value),
    )
    lot_a = along_z(lot_a)
    lot_b = in_plane(lot_b)
    lot_c = in_plane(lot_c)
    lot_b = along_z(repack_b(lot_b, cols, rank))
    moves = []
    for dz, i in place_all():
        to = dz * (each + EARLY)
        moves.append((i, to, dz, i * first, cols))
        moves.append((i, to + cols, dz, PLANE * first, rank))
        moves.append((i, to + each, dz, i * first + cols, EARLY))
    lot_a = repack(lot_a, moves, SIDE * (each + EARLY), PLANE)
    lot_a = in_plane(lot_a)
    moves = [(dz, i * rest, i, dz * rest, rest) for dz, i in place_all()]
    lot_c = repack(lot_c, moves, PLANE * rest, SIDE)
    lot_c = along_z(lot_c)
    mine, gains = collect(lot_b, cols, rank)
    theirs = lax.ppermute(mine, "model", [(m, m ^ 1) for m in range(models)])

    def adapter(refs, core, dz, i):
        at = (dz * PLANE + i) * rank
        own = lax.axis_index("model") % 2 == core
        return jnp.where(own, refs[0][at : at + rank, :], refs[1][at : at + rank, :])

    def value_of(refs, dz, i):
        weights = refs[dz][i * each : i * each + cols, :]
        return jnp.concatenate([weights, adapter(refs[SIDE:], 1, dz, i)], 0)

    def query_of(refs, dz, i):
        at = dz * (each + EARLY)
        return refs[i][at : at + each, :]

    def key_of(refs, dz, i):
        at = dz * (each + EARLY) + each
        early = refs[i][at : at + EARLY, :]
        late = refs[PLANE + dz][i * rest : (i + 1) * rest, :]
        return jnp.concatenate([early, late, adapter(refs[PLANE + SIDE :], 0, dz, i)], 0)

    final_v, scale_v = merge(value_of, 2, (*lot_b, mine, theirs), gains, mix)
    final_q, scale_q = merge(query_of, 0, lot_a, gains, mix)
    final_k, scale_k = merge(key_of, 1, (*lot_a, *lot_c, mine, theirs), gains, mix)
    return (
        final_q.T,
        final_k.T,
        final_v.T,
        scale_q.reshape(-1),
        scale_k.reshape(-1),
        scale_v.reshape(-1),
    )


def solution(mesh):
    return jax.shard_map(
        on_device,
        mesh=mesh,
        in_specs=(
            P("shard", "model"),
            P("shard", None),
            P(None, "model"),
            P("shard", "model"),
            P("shard", None),
            P(None, "model"),
            P("shard", "model"),
            P("shard", None),
            P(None, "model"),
            P("shard"),
        ),
        out_specs=(
            P(None, ("model", "shard")),
            P(None, ("model", "shard")),
            P(None, ("model", "shard")),
            P(("model", "shard")),
            P(("model", "shard")),
            P(("model", "shard")),
        ),
        check_vma=False,
    )
```

```python
import functools

import jax
import jax.numpy as jnp
from jax import lax
from jax.experimental import pallas as pl
from jax.experimental.pallas import tpu as pltpu
from jax.sharding import PartitionSpec as P


SIDE = 4
PLANE = 8
PEERS = SIDE * PLANE
GROUP = 4
LANES = 128
EARLY = 32
TAIL = 8
LATER_A = (0, 1, 3)
LATER_B = (0, 1, 2, 3, 6, 7)
HBM = pl.BlockSpec(memory_space=pltpu.HBM)
VMEM = pl.BlockSpec(memory_space=pltpu.VMEM)
PARAMS = pltpu.CompilerParams(vmem_limit_bytes=30 * 2**20)


def moved(place, dz, i):
    dy, dx = i // 2, i % 2
    z, y, x = place // PLANE, (place // 2) % SIDE, place % 2
    return ((z + dz) % SIDE) * PLANE + ((y + dy) % SIDE) * 2 + (x + dx) % 2


def came_from(place, dz, i):
    return moved(place, -dz % SIDE, (-(i // 2) % SIDE) * 2 + i % 2)


def far(x):
    return pltpu.with_memory_space_constraint(x, pltpu.HBM)


def shape(*dims):
    return jax.ShapeDtypeStruct(dims, jnp.bfloat16)


def split3(g):
    first = g.astype(jnp.bfloat16)
    rest = g - first.astype(jnp.float32)
    second = rest.astype(jnp.bfloat16)
    third = (rest - second.astype(jnp.float32)).astype(jnp.bfloat16)
    none = jnp.zeros((TAIL - 3, g.shape[1]), jnp.bfloat16)
    return jnp.concatenate([first, second, third, none], 0)


def low_of(core, lows, lowbox, sem):
    low_q, low_k, low_v = lows
    rank = low_q.shape[0]
    share = rank // 2
    even = pltpu.make_async_copy(low_k, lowbox.at[0:rank], sem.at[0])
    odd = pltpu.make_async_copy(low_v, lowbox.at[0:rank], sem.at[0])
    half = pltpu.make_async_copy(
        low_q.at[pl.ds(pl.multiple_of(core * share, share), share)],
        lowbox.at[rank : rank + share],
        sem.at[1],
    )
    half.start()

    @pl.when(core == 0)
    def _():
        even.start()

    @pl.when(core == 1)
    def _():
        odd.start()

    return even, half


def turned(block, cols):
    t = block.T
    return [t[p * cols : (p + 1) * cols, :] for p in range(GROUP)]


def fill_b(lot, dz, weights, cols):
    lot[dz * cols : (dz + 1) * cols, :] = weights


def fill_b_tail(lot, low, parts, cols):
    rank = low.shape[0]
    lot[SIDE * cols : SIDE * cols + rank, :] = low
    lot[SIDE * cols + rank :, :] = parts


def pack_first_kernel(wq, wk, wv, low_q, low_k, low_v, gain, lot_a, b4, b5, *refs, cols):
    inbox, vbox, turn, vturn, lowbox, gbox, insem, vsem, lowsem = refs
    wide = GROUP * cols
    first = cols + EARLY
    place = lax.axis_index("shard")
    core = lax.axis_index("model") % 2
    z, y, x = place // PLANE, (place // 2) % SIDE, place % 2
    copies = []
    for h in range(2):
        at = pl.multiple_of((((z + 2) % SIDE) * 2 + h) * wide, LANES)
        for m, w in enumerate((wq, wk)):
            copies.append(
                pltpu.make_async_copy(w.at[:, pl.ds(at, wide)], inbox.at[m, h], insem.at[m, h])
            )
            copies[-1].start()
    vcopies = []
    for dz in range(SIDE):
        at = pl.multiple_of((((z + dz) % SIDE) * 2 + ((y + 2) % SIDE) // 2) * wide, LANES)
        vcopies.append(pltpu.make_async_copy(wv.at[:, pl.ds(at, wide)], vbox.at[dz], vsem.at[dz]))
        vcopies[-1].start()
    small = [pltpu.make_async_copy(gain, gbox, lowsem.at[2])]
    small[0].start()
    small += low_of(core, (low_q, low_k, low_v), lowbox, lowsem)
    for copy in copies:
        copy.wait()
    for m in range(2):
        for h in range(2):
            for p, part in enumerate(turned(inbox[m, h], cols)):
                turn[h * GROUP + p, m * cols : (m + 1) * cols, :] = part
    for i in range(PLANE):
        to = moved(place, 0, i) % PLANE
        lot_a[i * first : (i + 1) * first, :] = turn[to, 0:first, :]
    for dz in range(SIDE):
        vcopies[dz].wait()
        for p, part in enumerate(turned(vbox[dz], cols)):
            vturn[dz * GROUP + p] = part
    for copy in small:
        copy.wait()
    parts = split3(gbox[...].reshape(1, -1))
    for dx, lot in enumerate((b4, b5)):
        for dz in range(SIDE):
            at = dz * GROUP + ((y + 2) % 2) * 2 + (x + dx) % 2
            fill_b(lot, dz, vturn[at], cols)
        fill_b_tail(lot, lowbox[...], parts, cols)


def pack_rest_kernel(wq, wk, wv, low_q, low_k, low_v, gain, *refs, cols):
    highs, refs = refs[:3], refs[3:]
    lot_a, refs = refs[: len(LATER_A)], refs[len(LATER_A) :]
    lot_b, refs = refs[: len(LATER_B)], refs[len(LATER_B) :]
    lot_c, mix, refs = refs[:PLANE], refs[PLANE], refs[PLANE + 1 :]
    inbox, turn, lowbox, gbox, highbox, insem, lowsem = refs
    wide = GROUP * cols
    first, rest = cols + EARLY, cols - EARLY
    width = wv.shape[1]
    place = lax.axis_index("shard")
    core = lax.axis_index("model") % 2
    start = place * cols
    base = jnp.minimum(start // LANES, width // LANES - 2) * LANES
    base = pl.multiple_of(base, LANES)
    copies = [
        [
            pltpu.make_async_copy(
                w.at[:, i * wide : (i + 1) * wide], inbox.at[m, i], insem.at[m, i]
            )
            for m, w in enumerate((wq, wk, wv))
        ]
        for i in range(PEERS // GROUP)
    ]
    for group in copies:
        for copy in group:
            copy.start()
    small = [
        pltpu.make_async_copy(high.at[:, pl.ds(base, 2 * LANES)], highbox.at[m], lowsem.at[3 + m])
        for m, high in enumerate(highs)
    ]
    small.append(pltpu.make_async_copy(gain, gbox, lowsem.at[2]))
    for copy in small:
        copy.start()
    small += low_of(core, (low_q, low_k, low_v), lowbox, lowsem)
    for i in range(PEERS // GROUP):
        for m in range(3):
            copies[i][m].wait()
            for p, part in enumerate(turned(inbox[m, i], cols)):
                turn[i * GROUP + p, m * cols : (m + 1) * cols, :] = part
    for copy in small:
        copy.wait()
    at_col = lax.broadcasted_iota(jnp.int32, (cols, 2 * LANES), 0) + (start - base)
    pick = at_col == lax.broadcasted_iota(jnp.int32, (cols, 2 * LANES), 1)
    pick = pick.astype(jnp.bfloat16)
    same = (
        lax.broadcasted_iota(jnp.int32, (cols, cols), 0)
        == lax.broadcasted_iota(jnp.int32, (cols, cols), 1)
    ).astype(jnp.bfloat16)
    for m in range(3):
        own = lax.dot_general(
            pick, highbox[m], (((1,), (1,)), ((), ())), preferred_element_type=jnp.float32
        )
        mix[m] = jnp.concatenate([same, own.astype(jnp.bfloat16)], 1)
    parts = split3(gbox[...].reshape(1, -1))
    for lot, i in zip(lot_b, LATER_B):
        for dz in range(SIDE):
            fill_b(lot, dz, turn[moved(place, dz, i), 2 * cols : 3 * cols, :], cols)
        fill_b_tail(lot, lowbox[...], parts, cols)
    for lot, dz in zip(lot_a, LATER_A):
        for i in range(PLANE):
            lot[i * first : (i + 1) * first, :] = turn[moved(place, dz, i), 0:first, :]
    for i in range(PLANE):
        for dz in range(SIDE):
            lot_c[i][dz * rest : (dz + 1) * rest, :] = turn[
                moved(place, dz, i), first : 2 * cols, :
            ]


def pack(weights, lows, gain, highs):
    rows, width = weights[0].shape
    rank = lows[0].shape[0]
    cols = width // PEERS
    groups = PEERS // GROUP
    wide = GROUP * cols
    passed = rank + rank // 2
    one_a = shape(PLANE * (cols + EARLY), rows)
    one_b = shape(SIDE * cols + passed + TAIL, rows)
    one_c = shape(SIDE * (cols - EARLY), rows)
    operands = [*map(far, weights), *map(far, lows), far(gain)]
    small = [
        pltpu.VMEM((passed, rows), jnp.bfloat16),
        pltpu.VMEM((rows,), jnp.float32),
    ]
    out = [one_a, one_b, one_b]
    lot_a, b4, b5 = pl.pallas_call(
        functools.partial(pack_first_kernel, cols=cols),
        in_specs=[HBM] * len(operands),
        out_specs=[VMEM] * len(out),
        out_shape=out,
        scratch_shapes=[
            pltpu.VMEM((2, 2, rows, wide), jnp.bfloat16),
            pltpu.VMEM((SIDE, rows, wide), jnp.bfloat16),
            pltpu.VMEM((PLANE, 2 * cols, rows), jnp.bfloat16),
            pltpu.VMEM((SIDE * GROUP, cols, rows), jnp.bfloat16),
            *small,
            pltpu.SemaphoreType.DMA((2, 2)),
            pltpu.SemaphoreType.DMA((SIDE,)),
            pltpu.SemaphoreType.DMA((3,)),
        ],
        compiler_params=PARAMS,
        name="pack_first",
    )(*operands)
    lots = {("a", 2): lot_a, ("b", 4): b4, ("b", 5): b5}
    operands += map(far, highs)
    names = [("a", k) for k in LATER_A] + [("b", k) for k in LATER_B]
    names += [("c", k) for k in range(PLANE)]
    out = [{"a": one_a, "b": one_b, "c": one_c}[name] for name, _ in names]
    out.append(shape(3, cols, cols + rank))
    *later, mix = pl.pallas_call(
        functools.partial(pack_rest_kernel, cols=cols),
        in_specs=[HBM] * len(operands),
        out_specs=[VMEM] * len(out),
        out_shape=out,
        scratch_shapes=[
            pltpu.VMEM((3, groups, rows, wide), jnp.bfloat16),
            pltpu.VMEM((PEERS, 3 * cols, rows), jnp.bfloat16),
            *small,
            pltpu.VMEM((3, rank, 2 * LANES), jnp.bfloat16),
            pltpu.SemaphoreType.DMA((3, groups)),
            pltpu.SemaphoreType.DMA((6,)),
        ],
        compiler_params=PARAMS,
        name="pack_rest",
    )(*operands)
    lots.update(zip(names, later))
    return (
        [lots["a", k] for k in range(SIDE)],
        [lots["b", k] for k in range(PLANE)],
        [lots["c", k] for k in range(PLANE)],
        mix,
    )


def repack_b(lot, cols, rank):
    rows = lot[0].shape[1]
    block = cols + rank
    tall = PLANE * block + 3 * PLANE

    def kernel(*refs):
        ins, outs = refs[:PLANE], refs[PLANE:]
        gains = [ref[SIDE * cols + rank :, :].astype(jnp.float32) for ref in ins]
        parts = [g[k : k + 1, :] for k in range(3) for g in gains]
        parts = jnp.concatenate(parts, 0).astype(jnp.bfloat16)
        for dz, out in enumerate(outs):
            for i, ref in enumerate(ins):
                at = i * block
                out[at : at + cols, :] = ref[dz * cols : (dz + 1) * cols, :]
                out[at + cols : at + block, :] = ref[SIDE * cols : SIDE * cols + rank, :]
            out[PLANE * block :, :] = parts

    return pl.pallas_call(
        kernel,
        in_specs=[VMEM] * PLANE,
        out_specs=[VMEM] * SIDE,
        out_shape=[shape(tall, rows)] * SIDE,
        compiler_params=PARAMS,
        name="repack_b",
    )(*lot)


def collect(lot, cols, rank):
    rows = lot[0].shape[1]
    block = cols + rank

    def kernel(*refs):
        ins, low, gain = refs[:SIDE], refs[SIDE], refs[SIDE + 1]
        for dz, ref in enumerate(ins):
            for i in range(PLANE):
                at = (dz * PLANE + i) * rank
                low[at : at + rank, :] = ref[i * block + cols : (i + 1) * block, :]
            g = ref[PLANE * block :, :].astype(jnp.float32)
            gain[dz * PLANE : (dz + 1) * PLANE, :] = (
                g[0:PLANE, :] + g[PLANE : 2 * PLANE, :] + g[2 * PLANE :, :]
            )

    return pl.pallas_call(
        kernel,
        in_specs=[VMEM] * SIDE,
        out_specs=[VMEM] * 2,
        out_shape=[shape(PEERS * rank, rows), jax.ShapeDtypeStruct((PEERS, rows), jnp.float32)],
        compiler_params=PARAMS,
        name="collect",
    )(*lot)


def repack(parts, moves, tall, count):
    def kernel(*refs):
        ins, outs = refs[: len(parts)], refs[len(parts) :]
        for k, to, j, at, n in moves:
            outs[k][to : to + n, :] = ins[j][at : at + n, :]

    out = [shape(tall, parts[0].shape[1])] * count
    return pl.pallas_call(
        kernel,
        in_specs=[VMEM] * len(parts),
        out_specs=[VMEM] * count,
        out_shape=out,
        compiler_params=PARAMS,
    )(*parts)


def place_all():
    return [(dz, i) for dz in range(SIDE) for i in range(PLANE)]


def merge(matrices, operands, gains, mix):
    _, cols, _ = mix.shape
    rows = gains.shape[1]
    count, many = len(operands), len(matrices)

    def kernel(*refs):
        ins, gain, both = refs[:count], refs[count], refs[count + 1]
        finals, scales = refs[count + 2 : count + 2 + many], refs[count + 2 + many :][:many]
        wide, outbox, outsem = refs[count + 2 + 2 * many :]
        place = lax.axis_index("shard")
        copies = []
        for k, (m, value_of) in enumerate(matrices):
            top = jnp.zeros((cols, rows), jnp.float32)
            for dz, i in place_all():
                at = dz * PLANE + i
                value = jnp.dot(both[m], value_of(ins, dz, i), preferred_element_type=jnp.float32)
                value = value * gain[at : at + 1, :]
                wide[came_from(place, dz, i)] = value
                top = jnp.maximum(top, jnp.abs(value))
            scale = jnp.max(top, axis=1, keepdims=True)
            scales[k][...] = jnp.broadcast_to(scale, (cols, LANES)).T[0:1, :]
            down = 1.0 / scale
            for c in range(cols // 32):
                part = slice(c * 32, (c + 1) * 32)
                for p in range(PEERS):
                    outbox[k, part, p * rows : (p + 1) * rows] = (
                        wide[p, part] * down[part]
                    ).astype(jnp.bfloat16)
                copies.append(
                    pltpu.make_async_copy(outbox.at[k, part], finals[k].at[part], outsem.at[k, c])
                )
                copies[-1].start()
        for copy in copies:
            copy.wait()

    return pl.pallas_call(
        kernel,
        in_specs=[VMEM] * (count + 2),
        out_specs=[HBM] * many + [VMEM] * many,
        out_shape=[shape(cols, PEERS * rows)] * many
        + [jax.ShapeDtypeStruct((1, cols), jnp.float32)] * many,
        scratch_shapes=[
            pltpu.VMEM((PEERS, cols, rows), jnp.float32),
            pltpu.VMEM((many, cols, PEERS * rows), jnp.bfloat16),
            pltpu.SemaphoreType.DMA((many, cols // 32)),
        ],
        compiler_params=PARAMS,
    )(*operands, gains, mix)


def on_device(
    w_query,
    low_query,
    high_query,
    w_key,
    low_key,
    high_key,
    w_value,
    low_value,
    high_value,
    norm_gain,
):
    cols = w_query.shape[1] // PEERS
    rank = low_query.shape[1]
    first, rest = cols + EARLY, cols - EARLY
    models = lax.axis_size("model")

    def leg(part, dz, i):
        pairs = [(s, moved(s, dz, i)) for s in range(PEERS)]
        return lax.ppermute(part, "shard", pairs)

    def along_z(lot):
        return [lot[0], *(leg(lot[dz], dz, 0) for dz in range(1, SIDE))]

    def in_plane(lot):
        return [lot[0], *(leg(lot[i], 0, i) for i in range(1, PLANE))]

    lot_a, lot_b, lot_c, mix = pack(
        (w_query, w_key, w_value),
        (low_query.T, low_key.T, low_value.T),
        norm_gain,
        (high_query, high_key, high_value),
    )
    lot_a = along_z(lot_a)
    lot_b = in_plane(lot_b)
    lot_c = in_plane(lot_c)
    passed = rank + rank // 2
    lot_b = along_z(repack_b(lot_b, cols, passed))
    moves = [(i, dz * first, dz, i * first, first) for dz, i in place_all()]
    lot_a = repack(lot_a, moves, SIDE * first, PLANE)
    lot_a = in_plane(lot_a)
    moves = [(dz, i * rest, i, dz * rest, rest) for dz, i in place_all()]
    lot_c = repack(lot_c, moves, PLANE * rest, SIDE)
    lot_c = along_z(lot_c)
    mine, gains = collect(lot_b, cols, passed)
    theirs = lax.ppermute(mine, "model", [(m, m ^ 1) for m in range(models)])

    def adapter(refs, core, dz, i, start, n):
        at = (dz * PLANE + i) * passed + start
        own = lax.axis_index("model") % 2 == core
        return jnp.where(own, refs[0][at : at + n, :], refs[1][at : at + n, :])

    def value_of(refs, dz, i):
        weights = refs[dz][i * (cols + passed) : i * (cols + passed) + cols, :]
        return jnp.concatenate([weights, adapter(refs[SIDE:], 1, dz, i, 0, rank)], 0)

    def query_of(refs, dz, i):
        weights = refs[i][dz * first : dz * first + cols, :]
        halves = [
            adapter(refs[PLANE + SIDE :], core, dz, i, rank, rank // 2) for core in range(2)
        ]
        return jnp.concatenate([weights, *halves], 0)

    def key_of(refs, dz, i):
        early = refs[i][dz * first + cols : (dz + 1) * first, :]
        late = refs[PLANE + dz][i * rest : (i + 1) * rest, :]
        low = adapter(refs[PLANE + SIDE :], 0, dz, i, 0, rank)
        return jnp.concatenate([early, late, low], 0)

    final_v, scale_v = merge([(2, value_of)], (*lot_b, mine, theirs), gains, mix)
    final_q, final_k, scale_q, scale_k = merge(
        [(0, query_of), (1, key_of)], (*lot_a, *lot_c, mine, theirs), gains, mix
    )
    return (
        final_q.T,
        final_k.T,
        final_v.T,
        scale_q.reshape(-1),
        scale_k.reshape(-1),
        scale_v.reshape(-1),
    )


def solution(mesh):
    return jax.shard_map(
        on_device,
        mesh=mesh,
        in_specs=(
            P("shard", "model"),
            P("shard", None),
            P(None, "model"),
            P("shard", "model"),
            P("shard", None),
            P(None, "model"),
            P("shard", "model"),
            P("shard", None),
            P(None, "model"),
            P("shard"),
        ),
        out_specs=(
            P(None, ("model", "shard")),
            P(None, ("model", "shard")),
            P(None, ("model", "shard")),
            P(("model", "shard")),
            P(("model", "shard")),
            P(("model", "shard")),
        ),
        check_vma=False,
    )
```
